32 devices in a mesh: dp: 2 (over core), seq: 4 (over z), tensor: 4 (over y, x).
Axes of the slice: x: 2, y: 2, z: 4, core: 2. Of those that a mesh axis runs over, the one named last changes fastest.
Arguments:
- tokens: bfloat16 [256, 4, 5120], P('seq', 'dp'), parts along dimension 1, may hold values from -6 to 6
- w_query: bfloat16 [5120, 5120], P(None, 'tensor'), may hold values from -0.5 to 0.5, as said below
- w_key: bfloat16 [5120, 5120], P(None, 'tensor'), may hold values from -0.5 to 0.5, as said below
- w_value: bfloat16 [5120, 5120], P(None, 'tensor'), may hold values from -0.078125 to 0.078125
- w_out: bfloat16 [5120, 5120], P('tensor'), may hold values from -0.125 to 0.125
- gain_query: float32 [5120], P('tensor'), may hold values from 0.5 to 4
- gain_key: float32 [5120], P('tensor'), may hold values from 0.5 to 4
Outputs:
- attended: bfloat16 [256, 4, 5120], P(('seq', 'tensor'), 'dp'), parts along dimension 1
The draws below stay inside these ranges and needn't reach their ends.
There are 2 independent parts, one for each index of `dp`. The reference program is written for one: setup_inputs(seed, part) draws one part's arguments, and reference() takes and returns one part's arrays. A program takes and returns all parts, laid end to end along the dimension named above; an argument that names none is the same for every part. Nothing has to cross between parts.
Inputs may be any that keep to these rules, and one draw needn't show every extreme that they name: `w_query`: entries of order 5120 ** -0.5 with unequal column scales. `w_key`: entries of order 5120 ** -0.5 with unequal column scales.
All inputs are finite; a program needn't handle non-finite values.
Results may differ from the reference program's by a relative error of at most 0.013.
The reference program's roundings to bfloat16 on the way count: a program that leaves them out, or rounds other values in their place, can miss the bound.
Values may be sent and summed in bfloat16 or wider, within the bound.
A program may use at most 256 MiB of HBM per device.

```python
import jax
import jax.numpy as jnp
from jax import lax

D = 5120
HEADS = 40
HEAD_DIM = 128
SEQS = 2
TOK_DEV = 64
SEQ = 256


def ramped_weight(key, salt):
    width = HEADS * HEAD_DIM
    first, second = jax.random.split(jax.random.fold_in(key, salt))
    base = jax.random.truncated_normal(first, -4.0, 4.0, (D, width), jnp.float32)
    heads = (jnp.arange(width) // HEAD_DIM).astype(jnp.float32)
    ramp = jnp.exp(jnp.log(0.6) + jnp.log(3.0) * heads / max(HEADS - 1, 1))
    upper = 3.3
    column = jnp.exp(jax.random.uniform(second, (width,), jnp.float32) * jnp.log(upper))
    scaled = base * (ramp * column)[None, :] / jnp.sqrt(jnp.float32(D))
    return jnp.clip(scaled, -0.5, 0.5).astype(jnp.bfloat16)


def drawn_gain(key, salt):
    width = HEADS * HEAD_DIM
    lower, upper = (0.5, 2.0)
    sample = jax.random.uniform(jax.random.fold_in(key, salt), (width,), jnp.float32, jnp.log(lower), jnp.log(upper))
    return jnp.exp(sample).astype(jnp.float32)


def draw_w_query(key, part):
    return ramped_weight(key, 11)


def draw_w_key(key, part):
    return ramped_weight(key, 23)


def draw_gain_query(key, part):
    return drawn_gain(key, 37)


def draw_gain_key(key, part):
    return drawn_gain(key, 41)


def with_spikes(entries, rng, source, target, parts, factor):
    def block_of(axis_at):
        return (jnp.arange(entries.shape[axis_at]) // (entries.shape[axis_at] // parts)).reshape((-1,) + (1,) * (entries.ndim - 1 - axis_at))

    one_side = jax.random.permutation(rng, parts)[block_of(target)]
    other_side = (block_of(target) + parts // 2) % parts
    return jnp.where((block_of(source) == one_side) | (block_of(source) == other_side), factor * entries, entries)


def steps_of(key, dims, shards, smallest, largest):
    level = 1.0
    for axis_at, parts in shards:
        heights = jax.random.uniform(jax.random.fold_in(jax.random.fold_in(key, 6), axis_at), (parts,), jnp.float32, smallest / len(shards), largest / len(shards))
        level = level * jnp.repeat(jnp.exp(heights), dims[axis_at] // parts).reshape((-1,) + (1,) * (len(dims) - 1 - axis_at))
    return level


def bell_draw(key, dims, spread, reach, cuts=(), held_as=jnp.bfloat16):
    loudness = steps_of(key, dims, cuts, -0.22, 0.18) if cuts else 1.0
    entries = jax.random.normal(key, dims, jnp.float32) * spread * loudness
    return jnp.minimum(jnp.maximum(entries, -reach), reach).astype(held_as)


def bell_draw_with(key, dims, scale, reach, cuts, heavy, kind=jnp.bfloat16):
    drawn = scale * jax.random.normal(key, dims, jnp.float32)
    if cuts:
        drawn = drawn * steps_of(key, dims, cuts, -0.22, 0.18)
    return jnp.clip(with_spikes(drawn, jax.random.fold_in(key, 3), *heavy), -reach, reach).astype(kind)


def setup_inputs(seed: int = 0, part: int = 0) -> dict:
    seeds = jax.random.split(jax.random.key(seed), 8)
    part_splits = jax.random.split(jax.random.fold_in(seeds[7], part), 8)
    return {
        "tokens": bell_draw(part_splits[0], (SEQ, SEQS, D), 1.0, 6.0, ((0, 4),)),
        "w_query": draw_w_query(jax.random.fold_in(seeds[7], 71), part),
        "w_key": draw_w_key(jax.random.fold_in(seeds[7], 71), part),
        "w_value": bell_draw(seeds[3], (D, HEADS * HEAD_DIM), D ** -0.5, 0.078125, ((1, 4),)),
        "w_out": bell_draw_with(seeds[4], (HEADS * HEAD_DIM, D), (HEADS * HEAD_DIM) ** -0.5, 0.125, ((0, 4),), (0, 1, 4, 2.0)),
        "gain_query": draw_gain_query(jax.random.fold_in(seeds[7], 71), part),
        "gain_key": draw_gain_key(jax.random.fold_in(seeds[7], 71), part),
    }


def rotary(field, positions):
    half = HEAD_DIM // 2
    shaped = field.reshape(field.shape[0], -1, HEAD_DIM)
    freqs = jnp.exp(-jnp.log(500000.0) * jnp.arange(half, dtype=jnp.float32) * 2.0 / HEAD_DIM)
    angle = positions.astype(jnp.float32)[:, None] * freqs[None, :]
    cosine = jnp.cos(angle)[:, None, :]
    sine = jnp.sin(angle)[:, None, :]
    first = shaped[..., :half]
    second = shaped[..., half:]
    turned = jnp.concatenate([first * cosine - second * sine, second * cosine + first * sine], axis=-1)
    return turned.reshape(field.shape[0], -1)

def one_sequence(seq_tokens, w_query, w_key, w_value, w_out, gain_query, gain_key):
    width = HEADS * HEAD_DIM
    query = jnp.dot(seq_tokens, w_query, preferred_element_type=jnp.float32)
    key_raw = jnp.dot(seq_tokens, w_key, preferred_element_type=jnp.float32)
    value = jnp.dot(seq_tokens, w_value, preferred_element_type=jnp.float32).astype(jnp.bfloat16)
    scale_q = lax.rsqrt(lax.optimization_barrier(jnp.sum(query * query, axis=1)) / width + 1e-06)
    scale_k = lax.rsqrt(lax.optimization_barrier(jnp.sum(key_raw * key_raw, axis=1)) / width + 1e-06)
    positions = jnp.arange(SEQ, dtype=jnp.int32)
    q_normed = rotary(query * scale_q[:, None] * gain_query[None, :], positions).astype(jnp.bfloat16)
    k_normed = rotary(key_raw * scale_k[:, None] * gain_key[None, :], positions).astype(jnp.bfloat16)
    keys_all = k_normed.reshape(SEQ, HEADS, HEAD_DIM).astype(jnp.float32)
    values_all = value.reshape(SEQ, HEADS, HEAD_DIM).astype(jnp.float32)
    factor = HEAD_DIM ** (-0.5)

    def one_block(index):
        start = (index * TOK_DEV).astype(jnp.int32)
        q_block = lax.dynamic_slice_in_dim(q_normed, start, TOK_DEV, 0).reshape(TOK_DEV, HEADS, HEAD_DIM).astype(jnp.float32)
        scores = jnp.einsum('qhd,khd->hqk', q_block, keys_all) * factor
        q_pos = start + jnp.arange(TOK_DEV, dtype=jnp.int32)
        allowed = positions[None, None, :] <= q_pos[None, :, None]
        top = lax.optimization_barrier(jnp.max(jnp.where(allowed, scores, -1e+30), axis=2))
        expo = jnp.where(allowed, jnp.exp(scores - top[..., None]), 0.0)
        total = lax.optimization_barrier(jnp.sum(expo, axis=2))
        rounded = expo.astype(jnp.bfloat16).astype(jnp.float32)
        summed = jnp.einsum('hqk,khd->hqd', rounded, values_all)
        mixed = (summed / total[..., None]).astype(jnp.bfloat16)
        return jnp.transpose(mixed, (1, 0, 2)).reshape(TOK_DEV, width)
    blocks = lax.map(one_block, jnp.arange(SEQ // TOK_DEV, dtype=jnp.int32))
    mixed_all = blocks.reshape(SEQ, width)
    return jnp.dot(mixed_all, w_out, preferred_element_type=jnp.float32).astype(jnp.bfloat16)

def reference(tokens, w_query, w_key, w_value, w_out, gain_query, gain_key):
    by_sequence = jnp.transpose(tokens, (1, 0, 2))

    def handle(seq_tokens):
        return one_sequence(seq_tokens, w_query, w_key, w_value, w_out, gain_query, gain_key)
    results = lax.map(handle, by_sequence)
    return jnp.transpose(results, (1, 0, 2))
```

```python
import functools

import jax
import jax.numpy as jnp
from jax import lax
from jax.experimental import pallas as pl
from jax.experimental.pallas import tpu as pltpu
from jax.sharding import PartitionSpec as P

HEADS = 40
HEAD_DIM = 128
MESH = pl.DeviceIdType.MESH
COLS = 2 * HEAD_DIM
RING = 5
F32 = jnp.float32
BF16 = jnp.bfloat16


def block_kernel(
    ns, nt, tok, width,
    x_ref, cos_ref, sin_ref, gq_ref, gk_ref, wq, wk, wv, wo,
    out_ref,
    ring, wov, sq, sk, sums_out, sums_in, rqs, rks,
    qbuf, kbuf, vbuf, own_o, own_lse, oout, lse_out, oin, lse_in,
    mixed, part, rs_in,
    w_sem, wo_sem, sum_send, sum_recv, k_send, k_recv, v_send, v_recv,
    q_send, q_recv, o_send, o_recv, l_send, l_recv, rs_send, rs_recv,
):
    dp = lax.axis_index("dp")
    z = lax.axis_index("seq")
    me = lax.axis_index("tensor")
    nc = qbuf.shape[0]
    rows = 2 * tok
    oc = wov.shape[2]
    no = wov.shape[0]

    def w_copy(kind, c, slot):
        ref = (wk, wq, wv)[kind]
        return pltpu.make_async_copy(
            ref.at[:, pl.ds(pl.multiple_of(c * COLS, COLS), COLS)], ring.at[slot], w_sem.at[slot]
        )

    def wo_copy(c):
        return pltpu.make_async_copy(
            wo.at[:, pl.ds(pl.multiple_of(c * oc, oc), oc)], wov.at[c], wo_sem.at[c]
        )

    def start(i):
        slot = lax.rem(i, RING)

        @pl.when((i < 2 * nc) & (lax.rem(i, 2) == 0))
        def _():
            w_copy(0, i // 2, slot).start()

        @pl.when((i < 2 * nc) & (lax.rem(i, 2) == 1))
        def _():
            w_copy(1, i // 2, slot).start()

        @pl.when((i >= 2 * nc) & (i < 3 * nc))
        def _():
            w_copy(2, i - 2 * nc, slot).start()

        @pl.when((i >= 3 * nc) & (i < 3 * nc + no))
        def _():
            wo_copy(i - 3 * nc).start()

    for i in range(RING - 1):
        w_copy(i % 2, i // 2, i).start()

    barrier = pltpu.get_barrier_semaphore()
    peers = []
    for dz in range(ns):
        for dk in range(nt):
            if dz or dk:
                peers.append((dp, lax.rem(z + dz, ns), lax.rem(me + dk, nt)))
    for peer in peers:
        pl.semaphore_signal(barrier, inc=1, device_id=peer, device_id_type=MESH)
    pl.semaphore_wait(barrier, len(peers))

    def remote(src, dst, ssem, rsem, to):
        return pltpu.make_async_remote_copy(
            src_ref=src, dst_ref=dst, send_sem=ssem, recv_sem=rsem, device_id=to, device_id_type=MESH
        )

    def k_copy(c, to):
        return remote(kbuf.at[c, :, pl.ds(0, tok)], kbuf.at[c, :, pl.ds(tok, tok)], k_send.at[c], k_recv.at[c], (dp, to, me))

    def v_copy(c, to):
        return remote(vbuf.at[c, :, pl.ds(0, tok)], vbuf.at[c, :, pl.ds(tok, tok)], v_send.at[c], v_recv.at[c], (dp, to, me))

    def q_copy(c, s, to):
        return remote(qbuf.at[c, :, pl.ds(0, tok)], qbuf.at[c, :, pl.ds(s * tok, tok)], q_send.at[s - 1, c], q_recv.at[s - 1, c], (dp, to, me))

    def o_copy(c, s, to):
        return remote(oout.at[s - 1, c], oin.at[s - 1, c], o_send.at[s - 1, c], o_recv.at[s - 1, c], (dp, to, me))

    def l_copy(s, to):
        return remote(lse_out.at[s - 1], lse_in.at[s - 1], l_send.at[s - 1], l_recv.at[s - 1], (dp, to, me))

    def product(kind, i):
        slot = lax.rem(i, RING)
        start(i + RING - 1)
        w_copy(kind, 0, slot).wait()
        return jnp.dot(x_ref[...], ring[slot], preferred_element_type=F32)

    def turned(acc, gain, c, buf):
        cosine, sine = cos_ref[...], sin_ref[...]
        for h in range(2):
            y = acc[:, h * HEAD_DIM : (h + 1) * HEAD_DIM] * gain[c, :, h * HEAD_DIM : (h + 1) * HEAD_DIM]
            y = (y * cosine + pltpu.roll(y, HEAD_DIM // 2, 1) * sine).astype(BF16)
            for j in range(2):
                buf[c, j, 0:tok, h * HEAD_DIM : (h + 1) * HEAD_DIM] = y[j * tok : (j + 1) * tok]

    sq[...] = jnp.zeros_like(sq)
    sk[...] = jnp.zeros_like(sk)

    @pl.loop(0, nc)
    def _(c):
        acc = product(0, 2 * c)
        sk[...] += acc[:, :HEAD_DIM] * acc[:, :HEAD_DIM] + acc[:, HEAD_DIM:] * acc[:, HEAD_DIM:]
        turned(acc, gk_ref, c, kbuf)

        @pl.when(z == 0)
        def _():
            k_copy(c, 1).start()

        acc = product(1, 2 * c + 1)
        sq[...] += acc[:, :HEAD_DIM] * acc[:, :HEAD_DIM] + acc[:, HEAD_DIM:] * acc[:, HEAD_DIM:]
        turned(acc, gq_ref, c, qbuf)

        @pl.when(z == 3)
        def _():
            q_copy(c, 2, 1).start()
            q_copy(c, 1, 2).start()

        @pl.when(z == 2)
        def _():
            q_copy(c, 1, 1).start()

    sums_out[...] = jnp.zeros_like(sums_out)
    sums_out[0:1, :] = jnp.sum(jnp.transpose(sq[...]), axis=0, keepdims=True)
    sums_out[1:2, :] = jnp.sum(jnp.transpose(sk[...]), axis=0, keepdims=True)
    mine = z * nt + me
    sends = []
    for n, peer in enumerate(peers):
        copy = remote(sums_out, sums_in.at[n], sum_send.at[n], sum_recv.at[n], peer)
        copy.start()
        sends.append(copy)

    @pl.loop(0, nc)
    def _(c):
        acc = product(2, 2 * nc + c).astype(BF16)
        for j in range(2):
            vbuf[c, j, 0:tok, :] = acc[j * tok : (j + 1) * tok]

        @pl.when(z == 0)
        def _():
            v_copy(c, 1).start()

    for c in range(max(0, RING - 1), no):
        wo_copy(c).start()

    for copy in sends:
        copy.wait()

    def total(back):
        tot = sums_out[...] if back == 0 else None
        n = 0
        for dz in range(ns):
            for dk in range(nt):
                if dz or dk:
                    if dz == back:
                        tot = sums_in[n] if tot is None else tot + sums_in[n]
                    n += 1
        return lax.rsqrt(tot / width + 1e-06)

    r0 = total(0)
    ahead = [r0, total(ns - 1), total(ns - 2)]
    factor = HEAD_DIM ** (-0.5)
    for s in range(3):
        rqs[s] = jnp.transpose(jnp.broadcast_to(ahead[s][0:1, :] * factor, (rows, rows)))
    r1 = total(1)
    low = lax.broadcasted_iota(jnp.int32, r0.shape, 1) < tok
    rks[0] = jnp.where(low, r0, pltpu.roll(r1, tok, 1))
    rks[1] = jnp.where(low, pltpu.roll(r0, tok, 1), r1)

    def attend(nq, nk, has_in):
        own_lse[...] = jnp.zeros_like(own_lse)
        if nq > 1:
            lse_out[...] = jnp.zeros_like(lse_out)
        lane = lax.broadcasted_iota(jnp.int32, (tok, HEAD_DIM), 1)
        row = lax.broadcasted_iota(jnp.int32, (tok, nk * tok), 0)
        col = lax.broadcasted_iota(jnp.int32, (tok, nk * tok), 1)
        allowed = (col <= row) | (col >= tok)

        @pl.loop(0, nc)
        def _(c):
            for s in range(1, nq):
                q_copy(c, s, z).wait_recv()
            if nk > 1:
                k_copy(c, z).wait_recv()
                v_copy(c, z).wait_recv()
            for j in range(2):
                for h in range(2):
                    hs = slice(h * HEAD_DIM, (h + 1) * HEAD_DIM)
                    u = c * 4 + j * 2 + h
                    k = kbuf[c, j, 0 : nk * tok, hs]
                    v = vbuf[c, j, 0 : nk * tok, hs]
                    q = qbuf[c, j, 0 : nq * tok, hs]
                    score = lax.dot_general(q, k, (((1,), (1,)), ((), ())), preferred_element_type=F32)
                    weights, tots, tops = [], [], []
                    for s in range(nq):
                        sc = score[s * tok : (s + 1) * tok]
                        sc = sc * rqs[s, j * tok : (j + 1) * tok, 0 : nk * tok] * rks[j, 1:2, 0 : nk * tok]
                        if s == 0:
                            sc = jnp.where(allowed, sc, -1e30)
                        top = jnp.max(sc, axis=1, keepdims=True)
                        e = jnp.exp(sc - top)
                        tots.append(jnp.sum(e, axis=1, keepdims=True))
                        tops.append(top)
                        weights.append(e.astype(BF16))
                    w = weights[0] if nq == 1 else jnp.concatenate(weights, axis=0)
                    acc = jnp.dot(w, v, preferred_element_type=F32)
                    for s in range(nq):
                        o = acc[s * tok : (s + 1) * tok] / tots[s]
                        if s == 0 and not has_in:
                            mixed[j * tok : (j + 1) * tok, pl.ds(pl.multiple_of(c * COLS + h * HEAD_DIM, HEAD_DIM), HEAD_DIM)] = o.astype(BF16)
                        elif s == 0:
                            own_o[c, j, :, hs] = o
                            own_lse[...] = jnp.where(lane == u, tops[s] + jnp.log(tots[s]), own_lse[...])
                        else:
                            oout[s - 1, c, j, :, hs] = o.astype(BF16)
                            lse_out[s - 1] = jnp.where(lane == u, tops[s] + jnp.log(tots[s]), lse_out[s - 1])
            for s in range(1, nq):
                o_copy(c, s, z + s).start()

        for s in range(1, nq):
            l_copy(s, z + s).start()

    def merge(ni):
        lane = lax.broadcasted_iota(jnp.int32, (tok, HEAD_DIM), 1)
        for s in range(1, ni + 1):
            l_copy(s, z).wait_recv()
        lses = [own_lse[...]] + [lse_in[s] for s in range(ni)]
        top = functools.reduce(jnp.maximum, lses)
        parts = [jnp.exp(v - top) for v in lses]
        tot = functools.reduce(jnp.add, parts)
        for s in range(ni + 1):
            rqs[s, 0:tok] = parts[s] / tot

        @pl.loop(0, nc)
        def _(c):
            for s in range(1, ni + 1):
                o_copy(c, s, z).wait_recv()
            for j in range(2):
                for h in range(2):
                    hs = slice(h * HEAD_DIM, (h + 1) * HEAD_DIM)
                    u = c * 4 + j * 2 + h
                    o = 0.0
                    for s in range(ni + 1):
                        share = jnp.sum(jnp.where(lane == u, rqs[s, 0:tok], 0.0), axis=1, keepdims=True)
                        o += share * (own_o[c, j, :, hs] if s == 0 else oin[s - 1, c, j, :, hs].astype(F32))
                    mixed[j * tok : (j + 1) * tok, pl.ds(pl.multiple_of(c * COLS + h * HEAD_DIM, HEAD_DIM), HEAD_DIM)] = o.astype(BF16)

    @pl.when(z == 0)
    def _():
        attend(1, 1, False)

    @pl.when(z == 1)
    def _():
        attend(3, 2, False)

    @pl.when(z == 2)
    def _():
        attend(2, 1, True)
        merge(1)

    @pl.when(z == 3)
    def _():
        attend(1, 1, True)
        merge(2)

    share = tok // nt

    def rs_copy(c, d):
        to = lax.rem(me + d, nt)
        return remote(
            part.at[c, :, pl.ds(pl.multiple_of(to * share, share), share)], rs_in.at[d - 1, c],
            rs_send.at[d - 1, c], rs_recv.at[d - 1, c], (dp, z, to),
        )

    @pl.loop(0, no)
    def _(c):
        wo_copy(c).wait()
        acc = jnp.dot(mixed[...], wov[c], preferred_element_type=F32).astype(BF16)
        for j in range(2):
            part[c, j] = acc[j * tok : (j + 1) * tok]
        for d in range(1, nt):
            rs_copy(c, d).start()

    @pl.loop(0, no)
    def _(c):
        for d in range(1, nt):
            rs_copy(c, d).wait_recv()
        for j in range(2):
            o = part[c, j, pl.ds(pl.multiple_of(me * share, share), share)].astype(F32)
            for d in range(1, nt):
                o += rs_in[d - 1, c, j].astype(F32)
            out_ref[j, :, pl.ds(pl.multiple_of(c * oc, oc), oc)] = o.astype(BF16)
        for d in range(1, nt):
            rs_copy(c, d).wait_send()

    @pl.loop(0, nc)
    def _(c):
        @pl.when(z == 0)
        def _():
            k_copy(c, 1).wait_send()
            v_copy(c, 1).wait_send()

        @pl.when(z == 3)
        def _():
            q_copy(c, 2, 1).wait_send()
            q_copy(c, 1, 2).wait_send()

        @pl.when(z == 2)
        def _():
            q_copy(c, 1, 1).wait_send()
            o_copy(c, 1, 3).wait_send()

        @pl.when(z == 1)
        def _():
            o_copy(c, 1, 2).wait_send()
            o_copy(c, 2, 3).wait_send()

    @pl.when(z == 2)
    def _():
        l_copy(1, 3).wait_send()

    @pl.when(z == 1)
    def _():
        l_copy(1, 2).wait_send()
        l_copy(2, 3).wait_send()


def fused(ns, nt, tokens, w_query, w_key, w_value, w_out, gain_query, gain_key):
    tok, seqs, depth = tokens.shape
    local = w_query.shape[1]
    nc = local // COLS
    oc = 1024
    no = depth // oc
    rows = tok * seqs
    width = HEADS * HEAD_DIM
    x = jnp.transpose(tokens, (1, 0, 2)).reshape(rows, depth)
    half = HEAD_DIM // 2
    freqs = jnp.exp(-jnp.log(500000.0) * jnp.arange(half, dtype=F32) * 2.0 / HEAD_DIM)
    positions = lax.axis_index("seq") * tok + jnp.arange(rows, dtype=jnp.int32) % tok
    angle = positions.astype(F32)[:, None] * freqs[None, :]
    cosine, sine = jnp.cos(angle), jnp.sin(angle)
    cosine = jnp.concatenate([cosine, cosine], axis=1)
    sine = jnp.concatenate([-sine, sine], axis=1)
    peers = ns * nt - 1
    vm = pltpu.VMEM
    dma = pltpu.SemaphoreType.DMA
    tile = (tok, HEAD_DIM)
    scratch = [
        vm((RING, depth, COLS), BF16), vm((no, local, oc), BF16),
        vm((rows, HEAD_DIM), F32), vm((rows, HEAD_DIM), F32),
        vm((8, rows), F32), vm((peers, 8, rows), F32),
        vm((3, rows, rows), F32), vm((2, 8, rows), F32),
        vm((nc, seqs, 3 * tok, COLS), BF16), vm((nc, seqs, 2 * tok, COLS), BF16), vm((nc, seqs, 2 * tok, COLS), BF16),
        vm((nc, seqs, tok, COLS), F32), vm(tile, F32),
        vm((2, nc, seqs, tok, COLS), BF16), vm((2,) + tile, F32),
        vm((2, nc, seqs, tok, COLS), BF16), vm((2,) + tile, F32),
        vm((rows, local), BF16), vm((no, seqs, tok, oc), BF16), vm((nt - 1, no, seqs, tok // nt, oc), BF16),
        dma((RING,)), dma((no,)), dma((peers,)), dma((peers,)),
        dma((nc,)), dma((nc,)), dma((nc,)), dma((nc,)),
        dma((2, nc)), dma((2, nc)), dma((2, nc)), dma((2, nc)), dma((2,)), dma((2,)),
        dma((nt - 1, no)), dma((nt - 1, no)),
    ]
    in_vmem = pl.BlockSpec(memory_space=pltpu.VMEM)
    anywhere = pl.BlockSpec(memory_space=pl.ANY)
    out = pl.pallas_call(
        functools.partial(block_kernel, ns, nt, tok, width),
        out_shape=jax.ShapeDtypeStruct((seqs, tok // nt, depth), BF16),
        in_specs=[in_vmem] * 5 + [anywhere] * 4,
        out_specs=in_vmem,
        scratch_shapes=scratch,
        compiler_params=pltpu.CompilerParams(collective_id=0, has_side_effects=True, vmem_limit_bytes=60 * 1024 * 1024),
    )(x, cosine, sine, gain_query.reshape(nc, 1, COLS), gain_key.reshape(nc, 1, COLS), w_query, w_key, w_value, w_out)
    return jnp.transpose(out, (1, 0, 2))


def rotary(field, positions):
    half = HEAD_DIM // 2
    shaped = field.reshape(field.shape[0], -1, HEAD_DIM)
    freqs = jnp.exp(-jnp.log(500000.0) * jnp.arange(half, dtype=jnp.float32) * 2.0 / HEAD_DIM)
    angle = positions.astype(jnp.float32)[:, None] * freqs[None, :]
    cosine = jnp.cos(angle)[:, None, :]
    sine = jnp.sin(angle)[:, None, :]
    first = shaped[..., :half]
    second = shaped[..., half:]
    turned = jnp.concatenate(
        [first * cosine - second * sine, second * cosine + first * sine], axis=-1
    )
    return turned.reshape(field.shape[0], -1)


def local(tokens, w_query, w_key, w_value, w_out, gain_query, gain_key):
    tok_rows = tokens.shape[0]
    seq_count = tokens.shape[1]
    local_width = w_query.shape[1]
    local_heads = local_width // HEAD_DIM
    width = HEADS * HEAD_DIM
    flat = tokens.reshape(tok_rows * seq_count, tokens.shape[2])
    query = jnp.dot(flat, w_query, preferred_element_type=jnp.float32)
    key_raw = jnp.dot(flat, w_key, preferred_element_type=jnp.float32)
    sum_query, sum_key = lax.psum(
        (jnp.sum(query * query, axis=1), jnp.sum(key_raw * key_raw, axis=1)), "tensor"
    )
    value = jnp.dot(flat, w_value, preferred_element_type=jnp.float32).astype(jnp.bfloat16)
    scale_q = lax.rsqrt(sum_query / width + 1e-06)
    scale_k = lax.rsqrt(sum_key / width + 1e-06)
    my_block = lax.axis_index("seq")
    positions = my_block * tok_rows + jnp.arange(tok_rows, dtype=jnp.int32)
    row_positions = (positions[:, None] + jnp.zeros((1, seq_count), jnp.int32)).reshape(-1)
    q_normed = rotary(query * scale_q[:, None] * gain_query[None, :], row_positions).astype(
        jnp.bfloat16
    )
    k_normed = rotary(key_raw * scale_k[:, None] * gain_key[None, :], row_positions).astype(
        jnp.bfloat16
    )
    q_heads = q_normed.reshape(tok_rows, seq_count, local_heads, HEAD_DIM)
    k_local = k_normed.reshape(tok_rows, seq_count, local_width)
    v_local = value.reshape(tok_rows, seq_count, local_width)
    factor = HEAD_DIM ** (-0.5)
    piece = (
        lax.all_gather(k_local, "seq", axis=0, tiled=True),
        lax.all_gather(v_local, "seq", axis=0, tiled=True),
    )
    key_pos = jnp.arange(piece[0].shape[0], dtype=jnp.int32)
    key_block = piece[0]
    count = key_block.shape[0]
    key_heads = key_block.reshape(count, seq_count, local_heads, HEAD_DIM)
    value_heads = piece[1].reshape(count, seq_count, local_heads, HEAD_DIM)
    scores = (
        jnp.einsum("qshd,kshd->shqk", q_heads, key_heads, preferred_element_type=jnp.float32)
        * factor
    )
    allowed = (key_pos[None, None, None, :] <= positions[None, None, :, None]) & (
        key_pos[None, None, None, :] >= 0
    )
    old_max = jnp.full((seq_count, local_heads, tok_rows), -1e30, jnp.float32)
    new_max = jnp.maximum(old_max, jnp.max(jnp.where(allowed, scores, -1e30), axis=3))
    expo = jnp.where(allowed, jnp.exp(scores - new_max[..., None]), 0.0)
    new_total = jnp.sum(expo, axis=3)
    added = jnp.einsum(
        "shqk,kshd->shqd",
        expo.astype(jnp.bfloat16),
        value_heads,
        preferred_element_type=jnp.float32,
    )
    final_state = (new_max, new_total, added)
    final_max, final_total, final_acc = final_state
    mixed = (final_acc / final_total[..., None]).astype(jnp.bfloat16)
    mixed = jnp.transpose(mixed, (2, 0, 1, 3)).reshape(tok_rows, seq_count, local_width)
    return lax.psum_scatter(
        jnp.dot(mixed, w_out, preferred_element_type=jnp.float32).astype(jnp.bfloat16),
        "tensor",
        scatter_dimension=0,
        tiled=True,
    )


def solution(mesh):
    ns, nt = mesh.shape["seq"], mesh.shape["tensor"]
    step = functools.partial(fused, ns, nt) if ns == 4 and nt == 4 else local
    return jax.shard_map(
        step,
        mesh=mesh,
        in_specs=(
            P("seq", "dp", None),
            P(None, "tensor"),
            P(None, "tensor"),
            P(None, "tensor"),
            P("tensor", None),
            P("tensor"),
            P("tensor"),
        ),
        out_specs=P(("seq", "tensor"), "dp", None),
        check_vma=False,
    )
```

```python
import functools

import jax
import jax.numpy as jnp
from jax import lax
from jax.experimental import pallas as pl
from jax.experimental.pallas import tpu as pltpu
from jax.sharding import PartitionSpec as P

HEADS = 40
HEAD_DIM = 128
MESH = pl.DeviceIdType.MESH
COLS = 2 * HEAD_DIM
RING = 9
F32 = jnp.float32
BF16 = jnp.bfloat16


def block_kernel(
    ns, nt, tok, width,
    x_ref, gq_in, gk_in, wq, wk, wv, wo,
    out_ref,
    ring, wov, cos_ref, sin_ref, gq_ref, gk_ref, sq, sk, sums_out, sums_in, rqs, rks,
    qbuf, kbuf, vbuf, own_o, own_lse, oout, lse_out, oin, lse_in,
    mixed, part, rs_in,
    w_sem, wo_sem, sum_send, sum_recv, k_send, k_recv, v_send, v_recv,
    q_send, q_recv, o_send, o_recv, l_send, l_recv, rs_send, rs_recv,
):
    dp = lax.axis_index("dp")
    z = lax.axis_index("seq")
    me = lax.axis_index("tensor")
    nc = qbuf.shape[0]
    rows = 2 * tok
    oc = wov.shape[2]
    no = wov.shape[0]

    def w_copy(kind, c, slot):
        ref = (wk, wq, wv)[kind]
        return pltpu.make_async_copy(
            ref.at[:, pl.ds(pl.multiple_of(c * COLS, COLS), COLS)], ring.at[slot], w_sem.at[slot]
        )

    def wo_copy(c):
        return pltpu.make_async_copy(
            wo.at[:, pl.ds(pl.multiple_of(c * oc, oc), oc)], wov.at[c], wo_sem.at[c]
        )

    def start(i):
        slot = lax.rem(i, RING)

        @pl.when((i < 2 * nc) & (lax.rem(i, 2) == 0))
        def _():
            w_copy(0, i // 2, slot).start()

        @pl.when((i < 2 * nc) & (lax.rem(i, 2) == 1))
        def _():
            w_copy(1, i // 2, slot).start()

        @pl.when((i >= 2 * nc) & (i < 3 * nc))
        def _():
            w_copy(2, i - 2 * nc, slot).start()

        @pl.when((i >= 3 * nc) & (i < 3 * nc + no))
        def _():
            wo_copy(i - 3 * nc).start()

    for i in range(RING - 1):
        w_copy(i % 2, i // 2, i).start()

    barrier = pltpu.get_barrier_semaphore()
    peers = []
    for dz in range(ns):
        for dk in range(nt):
            if dz or dk:
                peers.append((dp, lax.rem(z + dz, ns), lax.rem(me + dk, nt)))
    for peer in peers:
        pl.semaphore_signal(barrier, inc=1, device_id=peer, device_id_type=MESH)

    def remote(src, dst, ssem, rsem, to):
        return pltpu.make_async_remote_copy(
            src_ref=src, dst_ref=dst, send_sem=ssem, recv_sem=rsem, device_id=to, device_id_type=MESH
        )

    def k_copy(c, to):
        return remote(kbuf.at[c, :, pl.ds(0, tok)], kbuf.at[c, :, pl.ds(tok, tok)], k_send.at[c], k_recv.at[c], (dp, to, me))

    def v_copy(c, to):
        return remote(vbuf.at[c, :, pl.ds(0, tok)], vbuf.at[c, :, pl.ds(tok, tok)], v_send.at[c], v_recv.at[c], (dp, to, me))

    def q_copy(c, s, to):
        return remote(qbuf.at[c, :, pl.ds(0, tok)], qbuf.at[c, :, pl.ds(s * tok, tok)], q_send.at[s - 1, c], q_recv.at[s - 1, c], (dp, to, me))

    def o_copy(c, s, to):
        return remote(oout.at[s - 1, c], oin.at[s - 1, c], o_send.at[s - 1, c], o_recv.at[s - 1, c], (dp, to, me))

    def l_copy(s, to):
        return remote(lse_out.at[s - 1], lse_in.at[s - 1], l_send.at[s - 1], l_recv.at[s - 1], (dp, to, me))

    def product(kind, i):
        slot = lax.rem(i, RING)
        start(i + RING - 1)
        w_copy(kind, 0, slot).wait()
        return jnp.dot(x_ref[...], ring[slot], preferred_element_type=F32)

    def turned(acc, gain, c, buf):
        cosine, sine = cos_ref[...], sin_ref[...]
        for h in range(2):
            y = acc[:, h * HEAD_DIM : (h + 1) * HEAD_DIM] * gain[c, :, h * HEAD_DIM : (h + 1) * HEAD_DIM]
            y = (y * cosine + pltpu.roll(y, HEAD_DIM // 2, 1) * sine).astype(BF16)
            for j in range(2):
                buf[c, j, 0:tok, h * HEAD_DIM : (h + 1) * HEAD_DIM] = y[j * tok : (j + 1) * tok]

    lanes = lax.broadcasted_iota(jnp.int32, (tok, HEAD_DIM), 1)
    half = HEAD_DIM // 2
    freqs = jnp.exp(-jnp.log(500000.0) * lax.rem(lanes, half).astype(F32) * 2.0 / HEAD_DIM)
    spot = z * tok + lax.broadcasted_iota(jnp.int32, (tok, HEAD_DIM), 0)
    angle = spot.astype(F32) * freqs
    cosine = jnp.cos(angle)
    sine = jnp.sin(angle)
    sine = jnp.where(lanes < half, -sine, sine)
    for j in range(2):
        cos_ref[j * tok : (j + 1) * tok] = cosine
        sin_ref[j * tok : (j + 1) * tok] = sine
    for c in range(nc):
        gq_ref[c] = gq_in[c * COLS : (c + 1) * COLS].reshape(1, COLS)
        gk_ref[c] = gk_in[c * COLS : (c + 1) * COLS].reshape(1, COLS)
    sq[...] = jnp.zeros_like(sq)
    sk[...] = jnp.zeros_like(sk)

    @pl.loop(0, nc)
    def _(c):
        acc = product(0, 2 * c)

        @pl.when(c == 0)
        def _():
            pl.semaphore_wait(barrier, len(peers))

        sk[...] += acc[:, :HEAD_DIM] * acc[:, :HEAD_DIM] + acc[:, HEAD_DIM:] * acc[:, HEAD_DIM:]
        turned(acc, gk_ref, c, kbuf)

        @pl.when(z == 0)
        def _():
            k_copy(c, 1).start()

        acc = product(1, 2 * c + 1)
        sq[...] += acc[:, :HEAD_DIM] * acc[:, :HEAD_DIM] + acc[:, HEAD_DIM:] * acc[:, HEAD_DIM:]
        turned(acc, gq_ref, c, qbuf)

        @pl.when(z == 3)
        def _():
            q_copy(c, 2, 1).start()
            q_copy(c, 1, 2).start()

        @pl.when(z == 2)
        def _():
            q_copy(c, 1, 1).start()

    sums_out[...] = jnp.zeros_like(sums_out)
    sums_out[0:1, :] = jnp.sum(jnp.transpose(sq[...]), axis=0, keepdims=True)
    sums_out[1:2, :] = jnp.sum(jnp.transpose(sk[...]), axis=0, keepdims=True)
    mine = z * nt + me
    sends = []
    for n, peer in enumerate(peers):
        copy = remote(sums_out, sums_in.at[n], sum_send.at[n], sum_recv.at[n], peer)
        copy.start()
        sends.append(copy)

    def scales():
        for copy in sends:
            copy.wait()

        def total(back):
            tot = sums_out[...] if back == 0 else None
            n = 0
            for dz in range(ns):
                for dk in range(nt):
                    if dz or dk:
                        if dz == back:
                            tot = sums_in[n] if tot is None else tot + sums_in[n]
                        n += 1
            return lax.rsqrt(tot / width + 1e-06)

        r0 = total(0)
        ahead = [r0, total(ns - 1), total(ns - 2)]
        factor = HEAD_DIM ** (-0.5)
        for s in range(3):
            rqs[s] = jnp.transpose(jnp.broadcast_to(ahead[s][0:1, :] * factor, (rows, rows)))
        r1 = total(1)
        low = lax.broadcasted_iota(jnp.int32, r0.shape, 1) < tok
        rks[0] = jnp.where(low, r0, pltpu.roll(r1, tok, 1))
        rks[1] = jnp.where(low, pltpu.roll(r0, tok, 1), r1)

    lane = lax.broadcasted_iota(jnp.int32, (tok, HEAD_DIM), 1)

    def attend(c, nq, nk, has_in):
        row = lax.broadcasted_iota(jnp.int32, (tok, nk * tok), 0)
        col = lax.broadcasted_iota(jnp.int32, (tok, nk * tok), 1)
        allowed = (col <= row) | (col >= tok)
        for s in range(1, nq):
            q_copy(c, s, z).wait_recv()
        if nk > 1:
            k_copy(c, z).wait_recv()
            v_copy(c, z).wait_recv()
        for j in range(2):
            for h in range(2):
                hs = slice(h * HEAD_DIM, (h + 1) * HEAD_DIM)
                u = c * 4 + j * 2 + h
                k = kbuf[c, j, 0 : nk * tok, hs]
                v = vbuf[c, j, 0 : nk * tok, hs]
                q = qbuf[c, j, 0 : nq * tok, hs]
                score = lax.dot_general(q, k, (((1,), (1,)), ((), ())), preferred_element_type=F32)
                weights, tots, tops = [], [], []
                for s in range(nq):
                    sc = score[s * tok : (s + 1) * tok]
                    sc = sc * rqs[s, j * tok : (j + 1) * tok, 0 : nk * tok] * rks[j, 1:2, 0 : nk * tok]
                    if s == 0:
                        sc = jnp.where(allowed, sc, -1e30)
                    top = jnp.max(sc, axis=1, keepdims=True)
                    e = jnp.exp(sc - top)
                    tots.append(jnp.sum(e, axis=1, keepdims=True))
                    tops.append(top)
                    weights.append(e.astype(BF16))
                w = weights[0] if nq == 1 else jnp.concatenate(weights, axis=0)
                acc = jnp.dot(w, v, preferred_element_type=F32)
                for s in range(nq):
                    o = acc[s * tok : (s + 1) * tok] / tots[s]
                    if s == 0 and not has_in:
                        mixed[j * tok : (j + 1) * tok, pl.ds(pl.multiple_of(c * COLS + h * HEAD_DIM, HEAD_DIM), HEAD_DIM)] = o.astype(BF16)
                    elif s == 0:
                        own_o[c, j, :, hs] = o
                        own_lse[...] = jnp.where(lane == u, tops[s] + jnp.log(tots[s]), own_lse[...])
                    else:
                        oout[s - 1, c, j, :, hs] = o.astype(BF16)
                        lse_out[s - 1] = jnp.where(lane == u, tops[s] + jnp.log(tots[s]), lse_out[s - 1])
        for s in range(1, nq):
            o_copy(c, s, z + s).start()

    def merge(ni):
        for s in range(1, ni + 1):
            l_copy(s, z).wait_recv()
        lses = [own_lse[...]] + [lse_in[s] for s in range(ni)]
        top = functools.reduce(jnp.maximum, lses)
        parts = [jnp.exp(v - top) for v in lses]
        tot = functools.reduce(jnp.add, parts)
        for s in range(ni + 1):
            rqs[s, 0:tok] = parts[s] / tot

        @pl.loop(0, nc)
        def _(c):
            for s in range(1, ni + 1):
                o_copy(c, s, z).wait_recv()
            for j in range(2):
                for h in range(2):
                    hs = slice(h * HEAD_DIM, (h + 1) * HEAD_DIM)
                    u = c * 4 + j * 2 + h
                    o = 0.0
                    for s in range(ni + 1):
                        share = jnp.sum(jnp.where(lane == u, rqs[s, 0:tok], 0.0), axis=1, keepdims=True)
                        o += share * (own_o[c, j, :, hs] if s == 0 else oin[s - 1, c, j, :, hs].astype(F32))
                    mixed[j * tok : (j + 1) * tok, pl.ds(pl.multiple_of(c * COLS + h * HEAD_DIM, HEAD_DIM), HEAD_DIM)] = o.astype(BF16)

    own_lse[...] = jnp.zeros_like(own_lse)
    lse_out[...] = jnp.zeros_like(lse_out)

    @pl.loop(0, nc)
    def _(c):
        acc = product(2, 2 * nc + c).astype(BF16)
        for j in range(2):
            vbuf[c, j, 0:tok, :] = acc[j * tok : (j + 1) * tok]

        @pl.when(z == 0)
        def _():
            v_copy(c, 1).start()

        @pl.when(c == 0)
        def _():
            scales()

        @pl.when(z == 0)
        def _():
            attend(c, 1, 1, False)

        @pl.when(z == 1)
        def _():
            attend(c, 3, 2, False)

        @pl.when(z == 2)
        def _():
            attend(c, 2, 1, True)

        @pl.when(z == 3)
        def _():
            attend(c, 1, 1, True)

    @pl.when(z == 1)
    def _():
        l_copy(1, 2).start()
        l_copy(2, 3).start()

    @pl.when(z == 2)
    def _():
        l_copy(1, 3).start()
        merge(1)

    @pl.when(z == 3)
    def _():
        merge(2)

    share = tok // nt

    def rs_copy(c, d):
        to = lax.rem(me + d, nt)
        return remote(
            part.at[c, :, pl.ds(pl.multiple_of(to * share, share), share)], rs_in.at[d - 1, c],
            rs_send.at[d - 1, c], rs_recv.at[d - 1, c], (dp, z, to),
        )

    @pl.loop(0, no)
    def _(c):
        wo_copy(c).wait()
        acc = jnp.dot(mixed[...], wov[c], preferred_element_type=F32).astype(BF16)
        for j in range(2):
            part[c, j] = acc[j * tok : (j + 1) * tok]
        for d in range(1, nt):
            rs_copy(c, d).start()

    @pl.loop(0, no)
    def _(c):
        for d in range(1, nt):
            rs_copy(c, d).wait_recv()
        for j in range(2):
            o = part[c, j, pl.ds(pl.multiple_of(me * share, share), share)].astype(F32)
            for d in range(1, nt):
                o += rs_in[d - 1, c, j].astype(F32)
            out_ref[j, :, pl.ds(pl.multiple_of(c * oc, oc), oc)] = o.astype(BF16)
        for d in range(1, nt):
            rs_copy(c, d).wait_send()

    @pl.loop(0, nc)
    def _(c):
        @pl.when(z == 0)
        def _():
            k_copy(c, 1).wait_send()
            v_copy(c, 1).wait_send()

        @pl.when(z == 3)
        def _():
            q_copy(c, 2, 1).wait_send()
            q_copy(c, 1, 2).wait_send()

        @pl.when(z == 2)
        def _():
            q_copy(c, 1, 1).wait_send()
            o_copy(c, 1, 3).wait_send()

        @pl.when(z == 1)
        def _():
            o_copy(c, 1, 2).wait_send()
            o_copy(c, 2, 3).wait_send()

    @pl.when(z == 2)
    def _():
        l_copy(1, 3).wait_send()

    @pl.when(z == 1)
    def _():
        l_copy(1, 2).wait_send()
        l_copy(2, 3).wait_send()


def fused(ns, nt, tokens, w_query, w_key, w_value, w_out, gain_query, gain_key):
    tok, seqs, depth = tokens.shape
    local = w_query.shape[1]
    nc = local // COLS
    oc = 1024
    no = depth // oc
    rows = tok * seqs
    width = HEADS * HEAD_DIM
    x = jnp.transpose(tokens, (1, 0, 2)).reshape(rows, depth)
    peers = ns * nt - 1
    vm = pltpu.VMEM
    dma = pltpu.SemaphoreType.DMA
    tile = (tok, HEAD_DIM)
    scratch = [
        vm((RING, depth, COLS), BF16), vm((no, local, oc), BF16),
        vm((rows, HEAD_DIM), F32), vm((rows, HEAD_DIM), F32), vm((nc, 1, COLS), F32), vm((nc, 1, COLS), F32),
        vm((rows, HEAD_DIM), F32), vm((rows, HEAD_DIM), F32),
        vm((8, rows), F32), vm((peers, 8, rows), F32),
        vm((3, rows, rows), F32), vm((2, 8, rows), F32),
        vm((nc, seqs, 3 * tok, COLS), BF16), vm((nc, seqs, 2 * tok, COLS), BF16), vm((nc, seqs, 2 * tok, COLS), BF16),
        vm((nc, seqs, tok, COLS), F32), vm(tile, F32),
        vm((2, nc, seqs, tok, COLS), BF16), vm((2,) + tile, F32),
        vm((2, nc, seqs, tok, COLS), BF16), vm((2,) + tile, F32),
        vm((rows, local), BF16), vm((no, seqs, tok, oc), BF16), vm((nt - 1, no, seqs, tok // nt, oc), BF16),
        dma((RING,)), dma((no,)), dma((peers,)), dma((peers,)),
        dma((nc,)), dma((nc,)), dma((nc,)), dma((nc,)),
        dma((2, nc)), dma((2, nc)), dma((2, nc)), dma((2, nc)), dma((2,)), dma((2,)),
        dma((nt - 1, no)), dma((nt - 1, no)),
    ]
    in_vmem = pl.BlockSpec(memory_space=pltpu.VMEM)
    anywhere = pl.BlockSpec(memory_space=pl.ANY)
    out = pl.pallas_call(
        functools.partial(block_kernel, ns, nt, tok, width),
        out_shape=jax.ShapeDtypeStruct((seqs, tok // nt, depth), BF16),
        in_specs=[in_vmem] * 3 + [anywhere] * 4,
        out_specs=in_vmem,
        scratch_shapes=scratch,
        compiler_params=pltpu.CompilerParams(collective_id=0, has_side_effects=True, vmem_limit_bytes=60 * 1024 * 1024),
    )(x, gain_query, gain_key, w_query, w_key, w_value, w_out)
    return jnp.transpose(out, (1, 0, 2))


def rotary(field, positions):
    half = HEAD_DIM // 2
    shaped = field.reshape(field.shape[0], -1, HEAD_DIM)
    freqs = jnp.exp(-jnp.log(500000.0) * jnp.arange(half, dtype=jnp.float32) * 2.0 / HEAD_DIM)
    angle = positions.astype(jnp.float32)[:, None] * freqs[None, :]
    cosine = jnp.cos(angle)[:, None, :]
    sine = jnp.sin(angle)[:, None, :]
    first = shaped[..., :half]
    second = shaped[..., half:]
    turned = jnp.concatenate(
        [first * cosine - second * sine, second * cosine + first * sine], axis=-1
    )
    return turned.reshape(field.shape[0], -1)


def local(tokens, w_query, w_key, w_value, w_out, gain_query, gain_key):
    tok_rows = tokens.shape[0]
    seq_count = tokens.shape[1]
    local_width = w_query.shape[1]
    local_heads = local_width // HEAD_DIM
    width = HEADS * HEAD_DIM
    flat = tokens.reshape(tok_rows * seq_count, tokens.shape[2])
    query = jnp.dot(flat, w_query, preferred_element_type=jnp.float32)
    key_raw = jnp.dot(flat, w_key, preferred_element_type=jnp.float32)
    sum_query, sum_key = lax.psum(
        (jnp.sum(query * query, axis=1), jnp.sum(key_raw * key_raw, axis=1)), "tensor"
    )
    value = jnp.dot(flat, w_value, preferred_element_type=jnp.float32).astype(jnp.bfloat16)
    scale_q = lax.rsqrt(sum_query / width + 1e-06)
    scale_k = lax.rsqrt(sum_key / width + 1e-06)
    my_block = lax.axis_index("seq")
    positions = my_block * tok_rows + jnp.arange(tok_rows, dtype=jnp.int32)
    row_positions = (positions[:, None] + jnp.zeros((1, seq_count), jnp.int32)).reshape(-1)
    q_normed = rotary(query * scale_q[:, None] * gain_query[None, :], row_positions).astype(
        jnp.bfloat16
    )
    k_normed = rotary(key_raw * scale_k[:, None] * gain_key[None, :], row_positions).astype(
        jnp.bfloat16
    )
    q_heads = q_normed.reshape(tok_rows, seq_count, local_heads, HEAD_DIM)
    k_local = k_normed.reshape(tok_rows, seq_count, local_width)
    v_local = value.reshape(tok_rows, seq_count, local_width)
    factor = HEAD_DIM ** (-0.5)
    piece = (
        lax.all_gather(k_local, "seq", axis=0, tiled=True),
        lax.all_gather(v_local, "seq", axis=0, tiled=True),
    )
    key_pos = jnp.arange(piece[0].shape[0], dtype=jnp.int32)
    key_block = piece[0]
    count = key_block.shape[0]
    key_heads = key_block.reshape(count, seq_count, local_heads, HEAD_DIM)
    value_heads = piece[1].reshape(count, seq_count, local_heads, HEAD_DIM)
    scores = (
        jnp.einsum("qshd,kshd->shqk", q_heads, key_heads, preferred_element_type=jnp.float32)
        * factor
    )
    allowed = (key_pos[None, None, None, :] <= positions[None, None, :, None]) & (
        key_pos[None, None, None, :] >= 0
    )
    old_max = jnp.full((seq_count, local_heads, tok_rows), -1e30, jnp.float32)
    new_max = jnp.maximum(old_max, jnp.max(jnp.where(allowed, scores, -1e30), axis=3))
    expo = jnp.where(allowed, jnp.exp(scores - new_max[..., None]), 0.0)
    new_total = jnp.sum(expo, axis=3)
    added = jnp.einsum(
        "shqk,kshd->shqd",
        expo.astype(jnp.bfloat16),
        value_heads,
        preferred_element_type=jnp.float32,
    )
    final_state = (new_max, new_total, added)
    final_max, final_total, final_acc = final_state
    mixed = (final_acc / final_total[..., None]).astype(jnp.bfloat16)
    mixed = jnp.transpose(mixed, (2, 0, 1, 3)).reshape(tok_rows, seq_count, local_width)
    return lax.psum_scatter(
        jnp.dot(mixed, w_out, preferred_element_type=jnp.float32).astype(jnp.bfloat16),
        "tensor",
        scatter_dimension=0,
        tiled=True,
    )


def solution(mesh):
    ns, nt = mesh.shape["seq"], mesh.shape["tensor"]
    step = functools.partial(fused, ns, nt) if ns == 4 and nt == 4 else local
    return jax.shard_map(
        step,
        mesh=mesh,
        in_specs=(
            P("seq", "dp", None),
            P(None, "tensor"),
            P(None, "tensor"),
            P(None, "tensor"),
            P("tensor", None),
            P("tensor"),
            P("tensor"),
        ),
        out_specs=P(("seq", "tensor"), "dp", None),
        check_vma=False,
    )
```
